32 devices in a mesh: row: 2 (over core), col: 16 (over z, y, x).
Axes of the slice: x: 2, y: 2, z: 4, core: 2. Of those that a mesh axis runs over, the one named last changes fastest.
Arguments:
- embeddings: bfloat16 [256, 4096], P('col', 'row'), may hold values from -6 to 6
- slab_weight: bfloat16 [4096, 131072], P('row', 'col'), may hold values from -0.09375 to 0.09375
- target_table: bfloat16 [256, 131072], P(None, 'col'), may hold values from -6 to 6
- client_ids: int32 [256], replicated, may hold values from 0 to 255
- client_weights: float32 [256], replicated, may hold values from 0.1 to 1
Outputs:
- embed_grad: float32 [256, 4096], P('col', 'row')
- slab_grad: float32 [4096, 131072], P('row', 'col')
The draws below stay inside these ranges and needn't reach their ends.
Inputs may be any that keep to these rules, and one draw needn't show every extreme that they name: `client_ids`: table rows may repeat among clients.
All inputs are finite; a program needn't handle non-finite values.
Results may differ from the reference program's by a relative error of at most 0.0065.
Values may be sent and summed in bfloat16 or wider, within the bound.
A program may use at most 256 MiB of HBM per device.

```python
import math
import jax
import jax.numpy as jnp
from jax import lax

H = 4096
O = 131072
POOL = 256
B = 256
N_ROW = 2


def with_ends(result, rng, smallest, largest):
    place = [jax.random.randint(jax.random.fold_in(rng, axis), (), 0, length) for axis, length in enumerate(result.shape)]
    longest = result.shape.index(max(result.shape))
    neighbour = place[:longest] + [(place[longest] + 1) % result.shape[longest]] + place[longest + 1:]
    return result.at[tuple(place)].set(smallest).at[tuple(neighbour)].set(largest)


def level_of(stream_key, dims, pieces, low, high):
    factor_of, own = 1.0, jax.random.fold_in(stream_key, 6)
    for dim, shards_of in pieces:
        draws = jnp.exp(jax.random.uniform(jax.random.fold_in(own, dim), (shards_of,), jnp.float32, low / len(pieces), high / len(pieces)))
        factor_of = factor_of * jnp.repeat(draws, dims[dim] // shards_of).reshape([-1 if axis == dim else 1 for axis in range(len(dims))])
    return factor_of


def gaussian(key, dims, scale, most, cuts=(), held_as=jnp.bfloat16):
    loudness = level_of(key, dims, cuts, -0.22, 0.18) if cuts else 1.0
    array = jax.random.normal(key, dims, jnp.float32) * scale * loudness
    return jnp.minimum(jnp.maximum(array, -most), most).astype(held_as)


def setup_inputs(seed: int = 0) -> dict:
    key_of = jax.random.split(jax.random.key(seed), 6)
    embeddings = gaussian(key_of[0], (B, H), 1.0, 6.0, ((0, 16), (1, 2)))
    slab_weight = gaussian(key_of[1], (H, O), H ** -0.5, 0.09375, ((0, 2), (1, 16)))
    target_table = gaussian(key_of[2], (POOL, O), 1.0, 6.0, ((1, 16),))
    client_ids = with_ends(jax.random.randint(key_of[3], (B,), 0, POOL), jax.random.fold_in(key_of[3], 1), 0, POOL - 1).astype(jnp.int32)
    client_weights = jnp.clip(jnp.exp(jax.random.uniform(key_of[4], (B,), jnp.float32, math.log(0.1), math.log(1.0))), 0.1, 1.0)
    return {"embeddings": embeddings, "slab_weight": slab_weight, "target_table": target_table, "client_ids": client_ids, "client_weights": client_weights}


def reference(embeddings, slab_weight, target_table, client_ids, client_weights):
    block_width = embeddings.shape[1] // N_ROW
    emitted = jnp.zeros((embeddings.shape[0], slab_weight.shape[1]), jnp.float32)
    for group in range(N_ROW):
        partial_value = jnp.dot(embeddings[:, group * block_width:(group + 1) * block_width],
                          slab_weight[group * block_width:(group + 1) * block_width, :],
                          preferred_element_type=jnp.float32)
        rounded = lax.optimization_barrier(partial_value.astype(jnp.bfloat16))
        emitted = emitted + rounded.astype(jnp.float32)
    target = jnp.take(target_table, client_ids.astype(jnp.int32), axis=0).astype(jnp.float32)
    residual = (client_weights[:, None] * (emitted - target)).astype(jnp.bfloat16)
    embed_grad = lax.dot_general(residual, slab_weight, (((1,), (1,)), ((), ())),
                                 preferred_element_type=jnp.float32)
    slab_grad = lax.dot_general(embeddings, residual, (((0,), (0,)), ((), ())),
                                preferred_element_type=jnp.float32)
    return embed_grad, slab_grad
```

```python
import functools

import jax
import jax.numpy as jnp
from jax import lax
from jax.experimental import pallas as pl
from jax.experimental.pallas import tpu as pltpu
from jax.sharding import PartitionSpec as P

MESH = pl.DeviceIdType.MESH
CHUNKS = 4
VMEM_LIMIT = 67043328


def grid_of(mesh):
    n = mesh.shape["col"]
    try:
        spots = [d.coords for d in mesh.devices.flat]
        dims = [max(s[a] for s in spots) - min(s[a] for s in spots) + 1 for a in range(3)]
        if dims[0] * dims[1] * dims[2] == n:
            return dims[2], dims[1], dims[0]
    except AttributeError:
        pass
    return n, 1, 1


def tile_of(width):
    return 512 if width % 512 == 0 else width


def wide_of(width, most):
    wide = most
    while wide > tile_of(width) and width % wide:
        wide //= 2
    return max(wide, tile_of(width))


def front_kernel(grid, n_row, *refs):
    nz, ny, nx = grid
    n_out = ny * nx
    ids_ref, w_ref, emb_hbm, slab_hbm, table_hbm = refs[:5]
    res_out, feats_out = refs[5:7]
    part_outs = refs[7:7 + n_out]
    (feats, slab, table, acc, own, other, res, wcol, onehot, grad,
     slab_sem, load_sem, out_sem, gs_sem, gr_sem, xs_sem, xr_sem) = refs[7 + n_out:]
    chunks = feats.shape[0]
    rows, cw = feats.shape[4:]
    clients = nz * ny * nx * rows
    width = res.shape[1]
    tiles, _, tw = own.shape
    pool = table.shape[0]

    row, col = lax.axis_index("row"), lax.axis_index("col")
    z = lax.div(col, ny * nx)
    y = lax.rem(lax.div(col, nx), ny)
    x = lax.rem(col, nx)

    def at(z, y, x):
        return {"row": row, "col": (z * ny + y) * nx + x}

    def away(axis, k):
        if axis == "z":
            return at(lax.rem(z + k, nz), y, x)
        if axis == "y":
            return at(z, lax.rem(y + k, ny), x)
        return at(z, y, lax.rem(x + k, nx))

    size = {"z": nz, "y": ny, "x": nx}
    mates = [{"row": lax.rem(row + k, n_row), "col": col} for k in range(1, n_row)]
    peers = [away(a, k) for a in "zyx" for k in range(1, size[a])] + mates

    barrier = pltpu.get_barrier_semaphore()
    for peer in peers:
        pl.semaphore_signal(barrier, inc=1, device_id=peer, device_id_type=MESH)

    emb_loads = [
        pltpu.make_async_copy(emb_hbm.at[:, pl.ds(c * cw, cw)], feats.at[c, z, y, x], load_sem.at[c])
        for c in range(chunks)
    ]
    for load in emb_loads:
        load.start()
    table_load = pltpu.make_async_copy(table_hbm, table, load_sem.at[chunks])
    table_load.start()
    slab_loads = [
        pltpu.make_async_copy(slab_hbm.at[pl.ds(c * cw, cw)], slab.at[pl.ds(c * cw, cw)], slab_sem.at[c])
        for c in range(chunks)
    ]
    for load in slab_loads:
        load.start()
    pl.semaphore_wait(barrier, len(peers))
    for load in emb_loads:
        load.wait()

    def axes(c):
        return ("y", "x") if c % 2 == 0 else ("x", "y")

    def block(c, r, s):
        a, _ = axes(c)
        spot_y = lax.rem(y + s, ny) if a == "y" else y
        spot_x = lax.rem(x + s, nx) if a == "x" else x
        return feats.at[c, lax.rem(z + r, nz), spot_y, spot_x]

    def remote(ref, c, slot, axis, k):
        return pltpu.make_async_remote_copy(
            src_ref=ref, dst_ref=ref, send_sem=gs_sem.at[c, slot], recv_sem=gr_sem.at[c, slot],
            device_id=away(axis, k), device_id_type=MESH,
        )

    def z_copy(c, k):
        return remote(block(c, 0, 0), c, k - 1, "z", k)

    def a_copies(c, r):
        a, _ = axes(c)
        base = nz - 1 + r * (size[a] - 1)
        return [remote(block(c, r, 0), c, base + k - 1, a, k) for k in range(1, size[a])]

    def b_copies(c, r, s):
        a, b = axes(c)
        base = nz - 1 + nz * (size[a] - 1) + (r * size[a] + s) * (size[b] - 1)
        return [remote(block(c, r, s), c, base + k - 1, b, k) for k in range(1, size[b])]

    near = sorted(range(1, nz), key=lambda k: (min(k, nz - k), k))

    def pass_z(group):
        for k in near:
            for c in group:
                z_copy(c, k).wait_recv()
                for copy in a_copies(c, nz - k) + b_copies(c, nz - k, 0):
                    copy.start()

    def pass_a(group):
        for r in [0] + [nz - k for k in near]:
            for c in group:
                for k, arrived in enumerate(a_copies(c, r)):
                    arrived.wait_recv()
                    for copy in b_copies(c, r, size[axes(c)[0]] - 1 - k):
                        copy.start()

    def arrive(group):
        for c in group:
            for r in range(nz):
                for s in range(size[axes(c)[0]]):
                    for copy in b_copies(c, r, s):
                        copy.wait_recv()
            slab_loads[c].wait()
            feats_store(c).start()

    def gather_copies(c):
        found = [z_copy(c, k) for k in range(1, nz)]
        for r in range(nz):
            found += a_copies(c, r)
            for s in range(size[axes(c)[0]]):
                found += b_copies(c, r, s)
        return found

    for c in range(chunks):
        for copy in [z_copy(c, k) for k in near] + a_copies(c, 0) + b_copies(c, 0, 0):
            copy.start()

    hot = (lax.broadcasted_iota(jnp.int32, (pool, clients), 0) == ids_ref[...]).astype(jnp.float32)
    onehot[...] = hot.T.astype(jnp.bfloat16)
    wcol[...] = jnp.broadcast_to(w_ref[...], (128, clients)).T
    table_load.wait()

    def columns(i):
        return pl.ds(pl.multiple_of(i * tw, tw), tw)

    wide = wide_of(width, 2048)

    def stretch(i):
        return pl.ds(pl.multiple_of(i * wide, wide), wide)

    @pl.loop(0, width // wide)
    def _(i):
        res[:, stretch(i)] = jnp.dot(
            onehot[...], table[:, stretch(i)], preferred_element_type=jnp.float32
        ).astype(jnp.bfloat16)

    def features(c):
        return feats[c].reshape(clients, cw)

    def terms(group, cols):
        return sum(
            jnp.dot(features(c), slab[pl.ds(c * cw, cw), cols], preferred_element_type=jnp.float32) for c in group
        )

    def exchange(i):
        return [
            pltpu.make_async_remote_copy(
                src_ref=own.at[i], dst_ref=other.at[k, i],
                send_sem=xs_sem.at[k, i], recv_sem=xr_sem.at[k, i],
                device_id=mates[k], device_id_type=MESH,
            )
            for k in range(n_row - 1)
        ]

    def feats_store(c):
        return pltpu.make_async_copy(feats.at[c], feats_out.at[c], out_sem.at[c])

    early, late = range(chunks // 2), range(chunks // 2, chunks)
    pass_z(early)
    pass_a(early)
    pass_z(late)
    arrive(early)

    @pl.loop(0, width // wide)
    def _(i):
        acc[:, stretch(i)] = terms(early, stretch(i))

        @pl.when(i == 0)
        def _():
            pass_a(late)

    arrive(late)
    span = wide_of(width, 1024)
    per = span // tw

    @pl.loop(0, width // span)
    def _(i):
        @pl.when(i > 0)
        def _():
            for j in range(per):
                for copy in exchange(i * per - per + j):
                    copy.start()

        cols = pl.ds(pl.multiple_of(i * span, span), span)
        value = (acc[:, cols] + terms(late, cols)).astype(jnp.bfloat16)
        for j in range(per):
            own[i * per + j] = value[:, j * tw:(j + 1) * tw]

    for j in range(per):
        for copy in exchange(tiles - per + j):
            copy.start()

    weight = jnp.concatenate([wcol[...]] * (tw // 128), axis=1) if tw % 128 == 0 else wcol[:, :tw]

    def res_store(i):
        return pltpu.make_async_copy(res.at[:, columns(i)], res_out.at[:, columns(i)], out_sem.at[chunks + i])

    @pl.loop(0, tiles)
    def _(i):
        for copy in exchange(i):
            copy.wait_recv()
        total = own[i].astype(jnp.float32)
        for k in range(n_row - 1):
            total = total + other[k, i].astype(jnp.float32)
        total = total - res[:, columns(i)].astype(jnp.float32)
        res[:, columns(i)] = (weight * total).astype(jnp.bfloat16)

        @pl.when(i > 0)
        def _():
            res_store(i - 1).start()

    res_store(tiles - 1).start()

    hw = 256
    hidden = slab.shape[0]

    @pl.loop(0, hidden // hw)
    def _(j):
        cols = pl.ds(pl.multiple_of(j * hw, hw), hw)
        grad[...] = lax.dot_general(
            res[...], slab[cols, :], (((1,), (1,)), ((), ())), preferred_element_type=jnp.float32
        ).astype(jnp.bfloat16)
        for ky in range(ny):
            for kx in range(nx):
                there = lax.rem(y + ky, ny) * nx + lax.rem(x + kx, nx)
                for to_z in range(nz):
                    begin = pl.multiple_of((to_z * ny * nx + there) * rows, rows)
                    part_outs[ky * nx + kx][pl.ds(to_z * rows, rows), cols] = grad[pl.ds(begin, rows), :]

    for c in range(chunks):
        feats_store(c).wait()
        for copy in gather_copies(c):
            copy.wait_send()

    @pl.loop(0, tiles)
    def _(i):
        for copy in exchange(i):
            copy.wait_send()
        res_store(i).wait()


def front(grid, n_row, ids, weights, embeddings, slab_weight, table):
    nz, ny, nx = grid
    rows, hidden = embeddings.shape
    width = slab_weight.shape[1]
    pool = table.shape[0]
    clients = ids.shape[1]
    tw = tile_of(width)
    tiles = width // tw
    cw = hidden // CHUNKS
    peers = max(1, nz * ny * nx - 1)
    vmem = pl.BlockSpec(memory_space=pltpu.VMEM)
    anywhere = pl.BlockSpec(memory_space=pl.ANY)
    bf16, f32 = jnp.bfloat16, jnp.float32
    return pl.pallas_call(
        functools.partial(front_kernel, grid, n_row),
        out_shape=[
            jax.ShapeDtypeStruct((clients, width), bf16),
            jax.ShapeDtypeStruct((CHUNKS, nz, ny, nx, rows, cw), bf16),
        ] + [jax.ShapeDtypeStruct((nz * rows, hidden), bf16)] * (ny * nx),
        in_specs=[vmem, vmem, anywhere, anywhere, anywhere],
        out_specs=[anywhere, anywhere] + [vmem] * (ny * nx),
        scratch_shapes=[
            pltpu.VMEM((CHUNKS, nz, ny, nx, rows, cw), bf16),
            pltpu.VMEM((hidden, width), bf16),
            pltpu.VMEM((pool, width), bf16),
            pltpu.VMEM((clients, width), f32),
            pltpu.VMEM((tiles, clients, tw), bf16),
            pltpu.VMEM((n_row - 1, tiles, clients, tw), bf16),
            pltpu.VMEM((clients, width), bf16),
            pltpu.VMEM((clients, 128), f32),
            pltpu.VMEM((clients, pool), bf16),
            pltpu.VMEM((clients, 256), bf16),
            pltpu.SemaphoreType.DMA((CHUNKS,)),
            pltpu.SemaphoreType.DMA((CHUNKS + 1,)),
            pltpu.SemaphoreType.DMA((CHUNKS + tiles,)),
            pltpu.SemaphoreType.DMA((CHUNKS, peers)),
            pltpu.SemaphoreType.DMA((CHUNKS, peers)),
            pltpu.SemaphoreType.DMA((n_row - 1, tiles)),
            pltpu.SemaphoreType.DMA((n_row - 1, tiles)),
        ],
        compiler_params=pltpu.CompilerParams(
            collective_id=0, has_side_effects=True, vmem_limit_bytes=VMEM_LIMIT
        ),
        name="front",
    )(ids, weights, embeddings, slab_weight, table)


def slab_kernel(feats_ref, res_ref, *rest):
    out_ref, turned = rest[-2:]
    chunks, _, cw = feats_ref.shape

    @pl.when(pl.program_id(0) == 0)
    def _():
        for c in range(chunks):
            turned[pl.ds(c * cw, cw), :] = feats_ref[c].T

    out_ref[...] = jnp.dot(turned[...], res_ref[...], preferred_element_type=jnp.float32)


def slab_part(features, residual, before, first, last, hidden):
    chunks, clients, cw = features.shape
    width = residual.shape[1]
    tw = tile_of(width)
    in_specs = [
        pl.BlockSpec((chunks, clients, cw), lambda i: (0, 0, 0)),
        pl.BlockSpec((clients, tw), lambda i: (0, i + first)),
    ]
    args = [features, residual]
    aliases = {}
    if before is not None:
        in_specs.append(pl.BlockSpec(memory_space=pl.ANY))
        args.append(before)
        aliases = {2: 0}
    columns = (last - first) * tw
    return pl.pallas_call(
        slab_kernel,
        grid=(last - first,),
        out_shape=jax.ShapeDtypeStruct((hidden, width), jnp.float32),
        in_specs=in_specs,
        out_specs=pl.BlockSpec((hidden, tw), lambda i: (0, i + first)),
        scratch_shapes=[pltpu.VMEM((hidden, clients), jnp.bfloat16)],
        input_output_aliases=aliases,
        cost_estimate=pl.CostEstimate(
            flops=2 * hidden * clients * columns, bytes_accessed=4 * hidden * columns, transcendentals=0
        ),
        compiler_params=pltpu.CompilerParams(vmem_limit_bytes=40 * 1024 * 1024),
        name="slab_columns",
    )(*args)


def per_device(grid, n_row, embeddings, slab_weight, target_table, client_ids, client_weights):
    nz, ny, nx = grid
    rows, hidden = embeddings.shape
    clients = client_ids.shape[0]
    residual, feats, *parts = front(
        grid, n_row, client_ids.reshape(1, clients), client_weights.reshape(1, clients),
        embeddings, slab_weight, target_table,
    )
    features = feats.reshape(CHUNKS, clients, hidden // CHUNKS)
    width = slab_weight.shape[1]
    blocks = width // tile_of(width)
    cut = max(1, blocks * 9 // 16)

    def index(z, y, x):
        return ((z % nz) * ny + y % ny) * nx + x % nx

    spots = [(z, y, x) for z in range(nz) for y in range(ny) for x in range(nx)]
    total = parts[0].astype(jnp.float32)
    for ky in range(ny):
        for kx in range(nx):
            if ky or kx:
                perm = [(index(z, y, x), index(z, y + ky, x + kx)) for z, y, x in spots]
                total = total + lax.ppermute(parts[ky * nx + kx], "col", perm).astype(jnp.float32)
    slab_grad = slab_part(features, residual, None, 0, cut, hidden)

    total = total.reshape(nz, rows, hidden)
    here = lax.axis_index("col") // (ny * nx)
    embed_grad = lax.dynamic_index_in_dim(total, here, 0, keepdims=False)
    for kz in range(1, nz):
        perm = [(index(z, y, x), index(z + kz, y, x)) for z, y, x in spots]
        block = lax.dynamic_index_in_dim(total, (here + kz) % nz, 0, keepdims=False)
        embed_grad = embed_grad + lax.ppermute(block.astype(jnp.bfloat16), "col", perm).astype(jnp.float32)
    slab_grad = slab_part(features, residual, slab_grad, cut, blocks, hidden)
    return embed_grad, slab_grad


def solution(mesh):
    placed = (P("col", "row"), P("row", "col"), P(None, "col"), P(), P())
    return jax.shard_map(
        functools.partial(per_device, grid_of(mesh), mesh.shape["row"]),
        mesh=mesh,
        in_specs=placed,
        out_specs=(P("col", "row"), P("row", "col")),
        check_vma=False,
    )
```

```python
import functools

import jax
import jax.numpy as jnp
from jax import lax
from jax.experimental import pallas as pl
from jax.experimental.pallas import tpu as pltpu
from jax.sharding import PartitionSpec as P

MESH = pl.DeviceIdType.MESH
CHUNKS = 4
VMEM_LIMIT = 67043328


def grid_of(mesh):
    n = mesh.shape["col"]
    try:
        spots = [d.coords for d in mesh.devices.flat]
        dims = [max(s[a] for s in spots) - min(s[a] for s in spots) + 1 for a in range(3)]
        if dims[0] * dims[1] * dims[2] == n:
            return dims[2], dims[1], dims[0]
    except AttributeError:
        pass
    return n, 1, 1


def tile_of(width):
    return 512 if width % 512 == 0 else width


def wide_of(width, most):
    wide = most
    while wide > tile_of(width) and width % wide:
        wide //= 2
    return max(wide, tile_of(width))


def front_kernel(grid, n_row, *refs):
    nz, ny, nx = grid
    n_out = ny * nx
    ids_ref, w_ref, emb_hbm, slab_hbm, table_hbm = refs[:5]
    res_out, feats_out = refs[5:7]
    part_outs = refs[7:7 + n_out]
    (feats, slab, table, acc, own, other, res, wcol, onehot, grad,
     slab_sem, load_sem, out_sem, gs_sem, gr_sem, xs_sem, xr_sem) = refs[7 + n_out:]
    chunks = feats.shape[0]
    rows, cw = feats.shape[4:]
    clients = nz * ny * nx * rows
    width = res.shape[1]
    tiles, _, tw = own.shape
    pool = table.shape[0]

    row, col = lax.axis_index("row"), lax.axis_index("col")
    z = lax.div(col, ny * nx)
    y = lax.rem(lax.div(col, nx), ny)
    x = lax.rem(col, nx)

    def at(z, y, x):
        return {"row": row, "col": (z * ny + y) * nx + x}

    def away(axis, k):
        if axis == "z":
            return at(lax.rem(z + k, nz), y, x)
        if axis == "y":
            return at(z, lax.rem(y + k, ny), x)
        return at(z, y, lax.rem(x + k, nx))

    size = {"z": nz, "y": ny, "x": nx}
    mates = [{"row": lax.rem(row + k, n_row), "col": col} for k in range(1, n_row)]
    peers = [away(a, k) for a in "zyx" for k in range(1, size[a])] + mates

    barrier = pltpu.get_barrier_semaphore()
    for peer in peers:
        pl.semaphore_signal(barrier, inc=1, device_id=peer, device_id_type=MESH)

    emb_loads = [
        pltpu.make_async_copy(emb_hbm.at[:, pl.ds(c * cw, cw)], feats.at[c, z, y, x], load_sem.at[c])
        for c in range(chunks)
    ]
    for load in emb_loads:
        load.start()
    table_load = pltpu.make_async_copy(table_hbm, table, load_sem.at[chunks])
    table_load.start()
    slab_loads = [
        pltpu.make_async_copy(slab_hbm.at[pl.ds(c * cw, cw)], slab.at[pl.ds(c * cw, cw)], slab_sem.at[c])
        for c in range(chunks)
    ]
    pl.semaphore_wait(barrier, len(peers))
    for load in emb_loads:
        load.wait()

    def axes(c):
        return ("y", "x") if c % 2 == 0 else ("x", "y")

    def block(c, r, s):
        a, _ = axes(c)
        spot_y = lax.rem(y + s, ny) if a == "y" else y
        spot_x = lax.rem(x + s, nx) if a == "x" else x
        return feats.at[c, lax.rem(z + r, nz), spot_y, spot_x]

    def remote(ref, c, slot, axis, k):
        return pltpu.make_async_remote_copy(
            src_ref=ref, dst_ref=ref, send_sem=gs_sem.at[c, slot], recv_sem=gr_sem.at[c, slot],
            device_id=away(axis, k), device_id_type=MESH,
        )

    def z_copy(c, k):
        return remote(block(c, 0, 0), c, k - 1, "z", k)

    def a_copies(c, r):
        a, _ = axes(c)
        base = nz - 1 + r * (size[a] - 1)
        return [remote(block(c, r, 0), c, base + k - 1, a, k) for k in range(1, size[a])]

    def b_copies(c, r, s):
        a, b = axes(c)
        base = nz - 1 + nz * (size[a] - 1) + (r * size[a] + s) * (size[b] - 1)
        return [remote(block(c, r, s), c, base + k - 1, b, k) for k in range(1, size[b])]

    near = sorted(range(1, nz), key=lambda k: (min(k, nz - k), k))

    def pass_z(group):
        for k in near:
            for c in group:
                z_copy(c, k).wait_recv()
                for copy in a_copies(c, nz - k) + b_copies(c, nz - k, 0):
                    copy.start()

    def pass_a(group):
        for r in [0] + [nz - k for k in near]:
            for c in group:
                for k, arrived in enumerate(a_copies(c, r)):
                    arrived.wait_recv()
                    for copy in b_copies(c, r, size[axes(c)[0]] - 1 - k):
                        copy.start()

    def arrive(group):
        for c in group:
            for r in range(nz):
                for s in range(size[axes(c)[0]]):
                    for copy in b_copies(c, r, s):
                        copy.wait_recv()
            slab_loads[c].wait()
            feats_store(c).start()

    def gather_copies(c):
        found = [z_copy(c, k) for k in range(1, nz)]
        for r in range(nz):
            found += a_copies(c, r)
            for s in range(size[axes(c)[0]]):
                found += b_copies(c, r, s)
        return found

    for c in range(chunks):
        for copy in [z_copy(c, k) for k in near] + a_copies(c, 0) + b_copies(c, 0, 0):
            copy.start()

    for load in slab_loads:
        load.start()

    hot = (lax.broadcasted_iota(jnp.int32, (pool, clients), 0) == ids_ref[...]).astype(jnp.float32)
    onehot[...] = hot.T.astype(jnp.bfloat16)
    wcol[...] = jnp.broadcast_to(w_ref[...], (128, clients)).T
    table_load.wait()

    def columns(i):
        return pl.ds(pl.multiple_of(i * tw, tw), tw)

    wide = wide_of(width, 2048)

    def stretch(i):
        return pl.ds(pl.multiple_of(i * wide, wide), wide)

    @pl.loop(0, width // wide)
    def _(i):
        res[:, stretch(i)] = jnp.dot(
            onehot[...], table[:, stretch(i)], preferred_element_type=jnp.float32
        ).astype(jnp.bfloat16)

    def features(c):
        return feats[c].reshape(clients, cw)

    def terms(group, cols):
        return sum(
            jnp.dot(features(c), slab[pl.ds(c * cw, cw), cols], preferred_element_type=jnp.float32) for c in group
        )

    def exchange(i):
        return [
            pltpu.make_async_remote_copy(
                src_ref=own.at[i], dst_ref=other.at[k, i],
                send_sem=xs_sem.at[k, i], recv_sem=xr_sem.at[k, i],
                device_id=mates[k], device_id_type=MESH,
            )
            for k in range(n_row - 1)
        ]

    def feats_store(c):
        return pltpu.make_async_copy(feats.at[c], feats_out.at[c], out_sem.at[c])

    early, late = range(chunks // 2), range(chunks // 2, chunks)
    pass_z(early)
    pass_a(early)
    pass_z(late)
    arrive(early)

    @pl.loop(0, width // wide)
    def _(i):
        acc[:, stretch(i)] = terms(early, stretch(i))

        @pl.when(i == 0)
        def _():
            pass_a(late)

    arrive(late)
    span = wide_of(width, 1024)
    per = span // tw

    @pl.loop(0, width // span)
    def _(i):
        @pl.when(i > 0)
        def _():
            for j in range(per):
                for copy in exchange(i * per - per + j):
                    copy.start()

        cols = pl.ds(pl.multiple_of(i * span, span), span)
        value = (acc[:, cols] + terms(late, cols)).astype(jnp.bfloat16)
        for j in range(per):
            own[i * per + j] = value[:, j * tw:(j + 1) * tw]

    for j in range(per):
        for copy in exchange(tiles - per + j):
            copy.start()

    weight = jnp.concatenate([wcol[...]] * (tw // 128), axis=1) if tw % 128 == 0 else wcol[:, :tw]

    def res_store(i):
        return pltpu.make_async_copy(res.at[:, columns(i)], res_out.at[:, columns(i)], out_sem.at[chunks + i])

    @pl.loop(0, tiles)
    def _(i):
        for copy in exchange(i):
            copy.wait_recv()
        total = own[i].astype(jnp.float32)
        for k in range(n_row - 1):
            total = total + other[k, i].astype(jnp.float32)
        total = total - res[:, columns(i)].astype(jnp.float32)
        res[:, columns(i)] = (weight * total).astype(jnp.bfloat16)

        @pl.when(i > 0)
        def _():
            res_store(i - 1).start()

    res_store(tiles - 1).start()

    hidden = slab.shape[0]
    hw = grad.shape[1]

    @pl.loop(0, hidden // hw)
    def _(j):
        cols = pl.ds(pl.multiple_of(j * hw, hw), hw)
        grad[...] = lax.dot_general(
            res[...], slab[cols, :], (((1,), (1,)), ((), ())), preferred_element_type=jnp.float32
        ).astype(jnp.bfloat16)
        for ky in range(ny):
            for kx in range(nx):
                there = lax.rem(y + ky, ny) * nx + lax.rem(x + kx, nx)
                for to_z in range(nz):
                    begin = pl.multiple_of((to_z * ny * nx + there) * rows, rows)
                    part_outs[ky * nx + kx][pl.ds(to_z * rows, rows), cols] = grad[pl.ds(begin, rows), :]

    for c in range(chunks):
        feats_store(c).wait()
        for copy in gather_copies(c):
            copy.wait_send()

    @pl.loop(0, tiles)
    def _(i):
        for copy in exchange(i):
            copy.wait_send()
        res_store(i).wait()


def front(grid, n_row, ids, weights, embeddings, slab_weight, table):
    nz, ny, nx = grid
    rows, hidden = embeddings.shape
    width = slab_weight.shape[1]
    pool = table.shape[0]
    clients = ids.shape[1]
    tw = tile_of(width)
    tiles = width // tw
    cw = hidden // CHUNKS
    peers = max(1, nz * ny * nx - 1)
    vmem = pl.BlockSpec(memory_space=pltpu.VMEM)
    anywhere = pl.BlockSpec(memory_space=pl.ANY)
    bf16, f32 = jnp.bfloat16, jnp.float32
    return pl.pallas_call(
        functools.partial(front_kernel, grid, n_row),
        out_shape=[
            jax.ShapeDtypeStruct((clients, width), bf16),
            jax.ShapeDtypeStruct((CHUNKS, nz, ny, nx, rows, cw), bf16),
        ] + [jax.ShapeDtypeStruct((nz * rows, hidden), bf16)] * (ny * nx),
        in_specs=[vmem, vmem, anywhere, anywhere, anywhere],
        out_specs=[anywhere, anywhere] + [vmem] * (ny * nx),
        scratch_shapes=[
            pltpu.VMEM((CHUNKS, nz, ny, nx, rows, cw), bf16),
            pltpu.VMEM((hidden, width), bf16),
            pltpu.VMEM((pool, width), bf16),
            pltpu.VMEM((clients, width), f32),
            pltpu.VMEM((tiles, clients, tw), bf16),
            pltpu.VMEM((n_row - 1, tiles, clients, tw), bf16),
            pltpu.VMEM((clients, width), bf16),
            pltpu.VMEM((clients, 128), f32),
            pltpu.VMEM((clients, pool), bf16),
            pltpu.VMEM((clients, tile_of(hidden)), bf16),
            pltpu.SemaphoreType.DMA((CHUNKS,)),
            pltpu.SemaphoreType.DMA((CHUNKS + 1,)),
            pltpu.SemaphoreType.DMA((CHUNKS + tiles,)),
            pltpu.SemaphoreType.DMA((CHUNKS, peers)),
            pltpu.SemaphoreType.DMA((CHUNKS, peers)),
            pltpu.SemaphoreType.DMA((n_row - 1, tiles)),
            pltpu.SemaphoreType.DMA((n_row - 1, tiles)),
        ],
        compiler_params=pltpu.CompilerParams(
            collective_id=0, has_side_effects=True, vmem_limit_bytes=VMEM_LIMIT
        ),
        name="front",
    )(ids, weights, embeddings, slab_weight, table)


def slab_kernel(feats_ref, res_ref, *rest):
    out_ref, turned = rest[-2:]
    chunks, _, cw = feats_ref.shape

    @pl.when(pl.program_id(0) == 0)
    def _():
        for c in range(chunks):
            turned[pl.ds(c * cw, cw), :] = feats_ref[c].T

    out_ref[...] = jnp.dot(turned[...], res_ref[...], preferred_element_type=jnp.float32)


def slab_part(features, residual, before, first, last, hidden):
    chunks, clients, cw = features.shape
    width = residual.shape[1]
    tw = tile_of(width)
    in_specs = [
        pl.BlockSpec((chunks, clients, cw), lambda i: (0, 0, 0)),
        pl.BlockSpec((clients, tw), lambda i: (0, i + first)),
    ]
    args = [features, residual]
    aliases = {}
    if before is not None:
        in_specs.append(pl.BlockSpec(memory_space=pl.ANY))
        args.append(before)
        aliases = {2: 0}
    columns = (last - first) * tw
    return pl.pallas_call(
        slab_kernel,
        grid=(last - first,),
        out_shape=jax.ShapeDtypeStruct((hidden, width), jnp.float32),
        in_specs=in_specs,
        out_specs=pl.BlockSpec((hidden, tw), lambda i: (0, i + first)),
        scratch_shapes=[pltpu.VMEM((hidden, clients), jnp.bfloat16)],
        input_output_aliases=aliases,
        cost_estimate=pl.CostEstimate(
            flops=2 * hidden * clients * columns, bytes_accessed=4 * hidden * columns, transcendentals=0
        ),
        compiler_params=pltpu.CompilerParams(vmem_limit_bytes=40 * 1024 * 1024),
        name="slab_columns",
    )(*args)


def per_device(grid, n_row, embeddings, slab_weight, target_table, client_ids, client_weights):
    nz, ny, nx = grid
    rows, hidden = embeddings.shape
    clients = client_ids.shape[0]
    residual, feats, *parts = front(
        grid, n_row, client_ids.reshape(1, clients), client_weights.reshape(1, clients),
        embeddings, slab_weight, target_table,
    )
    features = feats.reshape(CHUNKS, clients, hidden // CHUNKS)
    width = slab_weight.shape[1]
    blocks = width // tile_of(width)
    cut = max(1, blocks * 9 // 16)

    def index(z, y, x):
        return ((z % nz) * ny + y % ny) * nx + x % nx

    spots = [(z, y, x) for z in range(nz) for y in range(ny) for x in range(nx)]
    total = parts[0].astype(jnp.float32)
    for ky in range(ny):
        for kx in range(nx):
            if ky or kx:
                perm = [(index(z, y, x), index(z, y + ky, x + kx)) for z, y, x in spots]
                total = total + lax.ppermute(parts[ky * nx + kx], "col", perm).astype(jnp.float32)
    slab_grad = slab_part(features, residual, None, 0, cut, hidden)

    total = total.reshape(nz, rows, hidden)
    here = lax.axis_index("col") // (ny * nx)
    embed_grad = lax.dynamic_index_in_dim(total, here, 0, keepdims=False)
    for kz in range(1, nz):
        perm = [(index(z, y, x), index(z + kz, y, x)) for z, y, x in spots]
        block = lax.dynamic_index_in_dim(total, (here + kz) % nz, 0, keepdims=False)
        embed_grad = embed_grad + lax.ppermute(block.astype(jnp.bfloat16), "col", perm).astype(jnp.float32)
    slab_grad = slab_part(features, residual, slab_grad, cut, blocks, hidden)
    return embed_grad, slab_grad


def solution(mesh):
    placed = (P("col", "row"), P("row", "col"), P(None, "col"), P(), P())
    return jax.shard_map(
        functools.partial(per_device, grid_of(mesh), mesh.shape["row"]),
        mesh=mesh,
        in_specs=placed,
        out_specs=(P("col", "row"), P("row", "col")),
        check_vma=False,
    )
```
